32 devices in a mesh: member: 2 (over x), wave: 16 (over z, y, core).
Axes of the slice: x: 2, y: 2, z: 4, core: 2. Of those that a mesh axis runs over, the one named last changes fastest.
Arguments:
- vorticity: bfloat16 [2560, 32, 1280], P(('member', 'wave')), parts along dimension 0, may hold values from -6 to 6
- divergence: bfloat16 [2560, 32, 1280], P(('member', 'wave')), parts along dimension 0, may hold values from -6 to 6
- legendre: bfloat16 [1280, 16, 1280], P('wave'), may hold values from -0.0068359375 to 0.0068359375
- wave_of_slot: int32 [1280], replicated, may hold values from 0 to 1279, as said below
- cycle_points: int32 [16], P('wave'), may hold values from 20 to 5136, as said below
- cos_squared: float32 [16], P('wave'), may hold values from 0.25 to 1
Outputs:
- grid: bfloat16 [32, 96, 5136], P(('member', 'wave')), parts along dimension 0
The draws below stay inside these ranges and needn't reach their ends.
There are 2 independent parts, one for each index of `member`. The reference program is written for one: setup_inputs(seed, part) draws one part's arguments, and reference() takes and returns one part's arrays. A program takes and returns all parts, laid end to end along the dimension named above; an argument that names none is the same for every part. Nothing has to cross between parts.
Inputs may be any that keep to these rules, and one draw needn't show every extreme that they name: `wave_of_slot`: each wavenumber appears in exactly one slot. `cycle_points`: every count is a multiple of 4; some cycle has 5136 points.
All inputs are finite; a program needn't handle non-finite values.
Results may differ from the reference program's by a relative error of at most 0.0063.
Values may be sent and summed in bfloat16 or wider, within the bound.
A program may use at most 192 MiB of HBM per device.

```python
import jax
import jax.numpy as jnp
from jax import lax

NWAVE = 1280
LEV = 16
NLON = 5136
NLAT_WIN = 16


def draw_wave_of_slot(key, part):
    return jax.random.permutation(key, NWAVE).astype(jnp.int32)


def draw_cycle_points(key, part):
    key_steps, key_place = jax.random.split(key)
    counts = jax.random.randint(key_steps, (NLAT_WIN,), 0, (NLON - 20) // 4 + 1, dtype=jnp.int32)
    widest = jax.random.randint(key_place, (), 0, NLAT_WIN, dtype=jnp.int32)
    based = 20 + 4 * counts
    return jnp.where(jnp.arange(NLAT_WIN, dtype=jnp.int32) == widest, NLON, based).astype(jnp.int32)


def level_of(key, extent, cuts, least, largest):
    gain, own = 1.0, jax.random.fold_in(key, 6)
    for dim, shards_of in cuts:
        draws = jnp.exp(jax.random.uniform(jax.random.fold_in(own, dim), (shards_of,), jnp.float32, least / len(cuts), largest / len(cuts)))
        gain = gain * jnp.repeat(draws, extent[dim] // shards_of).reshape([-1 if axis == dim else 1 for axis in range(len(extent))])
    return gain


def noise(own_key, extent, spread, bound, cuts=(), held_as=jnp.bfloat16):
    result = jax.random.normal(own_key, extent, jnp.float32) * spread
    if len(cuts) > 0:
        result = level_of(own_key, extent, cuts, -0.22, 0.18) * result
    return jnp.clip(result, min=-bound, max=bound).astype(held_as)


def setup_inputs(seed: int = 0, part: int = 0) -> dict:
    key_of = jax.random.split(jax.random.key(seed), 7)
    own_keys = jax.random.split(jax.random.fold_in(key_of[6], part), 7)
    vorticity = noise(own_keys[0], (NWAVE, 2 * LEV, NWAVE), 1.0, 6.0, ((0, 16),))
    divergence = noise(own_keys[1], (NWAVE, 2 * LEV, NWAVE), 1.0, 6.0, ((0, 16),))
    legendre = noise(key_of[2], (NWAVE, NLAT_WIN, NWAVE), (NWAVE * NWAVE // 2) ** -0.5, 0.0068359375, ((0, 16),))
    wave_of_slot = draw_wave_of_slot(jax.random.fold_in(key_of[6], 71), part)
    cycle_points = draw_cycle_points(jax.random.fold_in(key_of[6], 71), part)
    cos_squared = jnp.clip(0.25 + 0.75 * jax.random.uniform(key_of[5], (NLAT_WIN,), jnp.float32) ** level_of(key_of[5], (NLAT_WIN,), ((0, 16),), -0.2, 0.2), 0.25, 1.0)
    return dict(vorticity=vorticity, divergence=divergence, legendre=legendre, wave_of_slot=wave_of_slot, cycle_points=cycle_points, cos_squared=cos_squared)


def spectral_fields(zeta_in, delta_in, waves):
    columns = zeta_in.shape[-1]
    levels = zeta_in.shape[1] // 2
    degree = waves[:, None] + jnp.arange(columns, dtype=jnp.int32)[None, :]
    living = degree < NWAVE
    positive = living & (degree > 0)
    wave_f = waves.astype(jnp.float32)[:, None]
    degree_f = degree.astype(jnp.float32)
    radius = NWAVE / 4.0
    inverse = jnp.where(positive, -radius / jnp.maximum(degree_f * (degree_f + 1.0), 1.0), 0.0)
    quotient = jnp.maximum(degree_f * degree_f - wave_f * wave_f, 0.0) / jnp.maximum(4.0 * degree_f * degree_f - 1.0, 1.0)
    coupling = jnp.where(positive, jnp.sqrt(quotient), 0.0)
    coupling_next = jnp.concatenate([coupling[:, 1:], jnp.zeros_like(coupling[:, :1])], axis=1)
    upper_coef = ((degree_f + 2.0) * coupling_next)[:, None, :]
    lower_coef = ((degree_f - 1.0) * coupling)[:, None, :]
    live_mask = living.astype(jnp.float32)[:, None, :]
    zeta = zeta_in.astype(jnp.float32) * live_mask
    delta = delta_in.astype(jnp.float32) * live_mask
    stream = zeta * inverse[:, None, :]
    potential = delta * inverse[:, None, :]

    def meridional(values):
        shifted_up = jnp.concatenate([values[..., 1:], jnp.zeros_like(values[..., :1])], axis=-1)
        shifted_down = jnp.concatenate([jnp.zeros_like(values[..., :1]), values[..., :-1]], axis=-1)
        return (upper_coef * shifted_up - lower_coef * shifted_down) * live_mask
    stream_h = meridional(stream)
    potential_h = meridional(potential)
    wave_three = waves.astype(jnp.float32)[:, None, None]
    u_real = -wave_three * potential[:, levels:] - stream_h[:, :levels]
    u_imag = wave_three * potential[:, :levels] - stream_h[:, levels:]
    v_real = -wave_three * stream[:, levels:] + potential_h[:, :levels]
    v_imag = wave_three * stream[:, :levels] + potential_h[:, levels:]
    return jnp.concatenate([u_real, u_imag, v_real, v_imag, zeta, delta], axis=1).astype(jnp.bfloat16)

def derive(fourier, waves, cosine_sq):
    cycles, slots, columns = fourier.shape
    levels = columns // 8
    groups = fourier.reshape(cycles, slots, 4, 2, levels)
    wind_u = groups[:, :, 0]
    wind_v = groups[:, :, 1]
    zeta_f = groups[:, :, 2]
    delta_f = groups[:, :, 3]
    scale = (waves.astype(jnp.float32) / (NWAVE / 4.0))[None, :, None]
    u_lon = jnp.stack([-scale * wind_u[:, :, 1], scale * wind_u[:, :, 0]], axis=2)
    v_lon = jnp.stack([-scale * wind_v[:, :, 1], scale * wind_v[:, :, 0]], axis=2)
    factor = cosine_sq[:, None, None, None]
    u_lat = v_lon / factor - zeta_f
    v_lat = delta_f - u_lon / factor
    stacked = jnp.stack([wind_u, wind_v, u_lon, v_lon, u_lat, v_lat], axis=2)
    return stacked.reshape(cycles, slots, 12 * levels)

def cycle_basis(waves, points):
    positions = jnp.arange(NLON, dtype=jnp.int32)
    phase = waves[:, None] * positions[None, :] % points
    theta = 2.0 * jnp.pi / points.astype(jnp.float32) * phase.astype(jnp.float32)
    keeping = (2 * waves[:, None] < points) & (positions[None, :] < points)
    weight = jnp.where(waves == 0, 1.0, 2.0)[:, None]
    cosine = jnp.where(keeping, weight * jnp.cos(theta), 0.0)
    sine = jnp.where(keeping, -weight * jnp.sin(theta), 0.0)
    return jnp.stack([cosine, sine]).astype(jnp.bfloat16)

def reference(vorticity, divergence, legendre, wave_of_slot, cycle_points, cos_squared):
    blocks = NWAVE // 16

    def block_fourier(item):
        zeta_in, delta_in, values, waves = item
        spec = spectral_fields(zeta_in, delta_in, waves)
        return jnp.einsum('sck,slk->lsc', spec.astype(jnp.float32), values.astype(jnp.float32))
    items = (vorticity.reshape(blocks, 16, 2 * LEV, NWAVE), divergence.reshape(blocks, 16, 2 * LEV, NWAVE), legendre.reshape(blocks, 16, NLAT_WIN, NWAVE), wave_of_slot.reshape(blocks, 16))
    mapped = lax.map(block_fourier, items)
    fourier = jnp.transpose(mapped, (1, 0, 2, 3)).reshape(NLAT_WIN, NWAVE, 8 * LEV)
    fields = derive(fourier, wave_of_slot, cos_squared)

    def one_cycle(item):
        cycle_fields, points = item
        packed = cycle_fields.astype(jnp.bfloat16).reshape(NWAVE, 6, 2, LEV).astype(jnp.float32)
        basis = cycle_basis(wave_of_slot, points).astype(jnp.float32)
        summed = jnp.einsum('sfrl,rsp->flp', packed, basis)
        return summed.reshape(6 * LEV, NLON).astype(jnp.bfloat16)
    return lax.map(one_cycle, (fields, cycle_points))
```

```python
import functools

import jax
import jax.numpy as jnp
from jax import lax
from jax.experimental import pallas as pl
from jax.experimental.pallas import tpu as pltpu
from jax.sharding import PartitionSpec as P

NLON = 5136
LANES = 128
COS = (1.0, -1 / 2, 1 / 24, -1 / 720, 1 / 40320, -1 / 3628800, 1 / 479001600,
       -1 / 87178291200, 1 / 20922789888000, -1 / 6402373705728000)
SIN = (1.0, -1 / 6, 1 / 120, -1 / 5040, 1 / 362880, -1 / 39916800, 1 / 6227020800,
       -1 / 1307674368000, 1 / 355687428096000, -1 / 121645100408832000)


def slot_block(slots):
    return max(b for b in range(1, 9) if slots % b == 0)


def degree_coefs(wave, count):
    degree = wave + lax.broadcasted_iota(jnp.int32, (wave.shape[0], count), 1)
    living = degree < count
    positive = living & (degree > 0)
    m = wave.astype(jnp.float32)
    n = degree.astype(jnp.float32)
    inverse = jnp.where(positive, -(count / 4.0) / jnp.maximum(n * (n + 1.0), 1.0), 0.0)

    def eps(x):
        return jnp.sqrt(jnp.maximum(x * x - m * m, 0.0) / jnp.maximum(4.0 * x * x - 1.0, 1.0))

    lower = jnp.where(positive, eps(n), 0.0)
    upper = jnp.where(degree + 1 < count, eps(n + 1.0), 0.0)
    live = living.astype(jnp.float32)
    return live, inverse * m, inverse * (n + 1.0) * lower, -inverse * n * upper


def slot_fourier(values, live, along, before, after, zd):
    count = values.shape[-1]
    p = values.astype(jnp.float32)
    lon = p * along
    lat = pltpu.roll(p, 1, 1) * before + pltpu.roll(p, count - 1, 1) * after
    left = jnp.concatenate([p * live, lon, lat], axis=0).astype(jnp.bfloat16)
    sums = lax.dot_general(left, zd, (((1,), (1,)), ((), ())), preferred_element_type=jnp.float32)
    rows = p.shape[0]
    lev = zd.shape[0] // 4
    plain, a, b = sums[:rows], sums[rows : 2 * rows], sums[2 * rows :]
    zr, zi, dr, di = (slice(g * lev, (g + 1) * lev) for g in range(4))
    turned = jnp.concatenate([-a[:, di], a[:, dr], -a[:, zi], a[:, zr]], axis=1)
    lane = lax.broadcasted_iota(jnp.int32, b.shape, 1)
    winds = turned + jnp.where(lane < 2 * lev, -b, b)
    return jnp.concatenate([winds, plain], axis=1)


def legendre_kernel(wave_ref, zeta_ref, delta_ref, values_ref, out_ref):
    count = zeta_ref.shape[-1]
    coefs = degree_coefs(wave_ref[0], count)
    for s in range(zeta_ref.shape[0]):
        zd = jnp.concatenate([zeta_ref[s], delta_ref[s]], axis=0)
        out = slot_fourier(values_ref[s], *(c[s : s + 1] for c in coefs), zd)
        out_ref[s] = out.astype(out_ref.dtype)


def legendre_sums(waves, vorticity, divergence, legendre):
    slots, columns, count = vorticity.shape
    cycles = legendre.shape[1]
    sb = slot_block(slots)
    block = lambda rows: pl.BlockSpec((sb, rows, count), lambda i: (i, 0, 0))
    return pl.pallas_call(
        legendre_kernel,
        grid=(slots // sb,),
        in_specs=[
            pl.BlockSpec((1, sb, 1), lambda i: (i, 0, 0)),
            block(columns),
            block(columns),
            block(cycles),
        ],
        out_specs=pl.BlockSpec((sb, cycles, 4 * columns), lambda i: (i, 0, 0)),
        out_shape=jax.ShapeDtypeStruct((slots, cycles, 4 * columns), jnp.bfloat16),
    )(waves.reshape(slots // sb, sb, 1), vorticity, divergence, legendre)


def horner(coefs, x):
    total = jnp.full_like(x, coefs[-1])
    for c in coefs[-2::-1]:
        total = total * x + c
    return total


def turn(steps, points, per_point):
    turns = jnp.round(steps * per_point)
    theta = (steps - turns * points) * (per_point * (2.0 * jnp.pi))
    square = theta * theta
    return horner(COS, square), theta * horner(SIN, square)


def fill_basis(row, points, basis):
    slots = row.shape[1]
    tiles = basis.shape[1] // LANES
    per_point = 1.0 / points
    column = lambda x: jnp.broadcast_to(x, (LANES, slots)).T
    wave = column(row)
    step_c, step_s = (column(x) for x in turn(row * float(LANES), points, per_point))
    lane = lax.broadcasted_iota(jnp.int32, (16, LANES), 1).astype(jnp.float32)
    for start in range(0, slots, 16):
        rows = slice(start, start + 16)
        c, s = turn(wave[rows] * lane, points, per_point)
        cs, ss = step_c[rows], step_s[rows]
        for t in range(tiles):
            at = slice(t * LANES, (t + 1) * LANES)
            basis[rows, at] = c.astype(basis.dtype)
            basis[slots + start : slots + start + 16, at] = s.astype(basis.dtype)
            c, s = c * cs - s * ss, s * cs + c * ss


def fill_fields(arrived, wave, points, cosine_sq, count, packed):
    x = arrived.astype(jnp.float32).T
    lev = x.shape[0] // 8
    ur, ui, vr, vi, zr, zi, dr, di = (x[g * lev : (g + 1) * lev] for g in range(8))
    slots = wave.shape[1]
    m = wave.astype(jnp.float32)
    q = m * (4.0 / count)
    over = 1.0 / jnp.full_like(m, cosine_sq)
    ulr, uli, vlr, vli = -q * ui, q * ur, -q * vi, q * vr
    fields = (
        (ur, ui), (vr, vi), (ulr, uli), (vlr, vli),
        (vlr * over - zr, vli * over - zi), (dr - ulr * over, di - uli * over),
    )
    weight = jnp.where(2 * wave < points, jnp.where(wave == 0, 1.0, 2.0), 0.0)
    for f, (re, im) in enumerate(fields):
        a, b = re * weight, -im * weight
        for j in range(4):
            phase = (wave * j) & 3
            c = jnp.where(phase == 0, 1.0, jnp.where(phase == 2, -1.0, 0.0))
            s = jnp.where(phase == 1, 1.0, jnp.where(phase == 3, -1.0, 0.0))
            start = (j * len(fields) + f) * lev
            rows = slice(start, start + lev)
            packed[rows, :slots] = (a * c + b * s).astype(packed.dtype)
            packed[rows, slots:] = (b * c - a * s).astype(packed.dtype)


def place(quarters, points, line):
    rows = quarters.shape[0] // 4
    tiles = quarters.shape[1] // LANES
    quarter = points // 4
    lane = lax.broadcasted_iota(jnp.int32, (rows, LANES), 1)
    line[...] = jnp.zeros_like(line)
    for j in range(4):
        offset = quarter * j
        base = pl.multiple_of(offset // LANES * LANES, LANES)
        shift = offset - base
        previous = jnp.zeros((rows, LANES), jnp.float32)
        for t in range(tiles + 1):
            rolled = jnp.zeros((rows, LANES), jnp.float32)
            if t < tiles:
                tile = quarters[j * rows : (j + 1) * rows, t * LANES : (t + 1) * LANES]
                tile = jnp.where(lane + t * LANES < quarter, tile.astype(jnp.float32), 0.0)
                rolled = pltpu.roll(tile, shift, 1)
            moved = jnp.where(lane < shift, previous, rolled).astype(line.dtype)
            at = pl.ds(pl.multiple_of(base + t * LANES, LANES), LANES)
            line[:, at] = line[:, at] + moved
            previous = rolled


def synthesis_kernel(count, points_ref, cosine_ref, wave_ref, arrived_ref, out_ref, basis, packed, quarters, line):
    cycle = pl.program_id(0)
    points = points_ref[cycle]
    wave = wave_ref[...]
    points_f = jnp.full(wave.shape, points, jnp.int32).astype(jnp.float32)
    fill_basis(wave.astype(jnp.float32), points_f[:1, :1], basis)
    fill_fields(arrived_ref[0], wave, points, cosine_ref[cycle], count, packed)
    width = quarters.shape[1]
    for start in range(0, width, 256):
        at = slice(start, min(start + 256, width))
        quarters[:, at] = jnp.dot(
            packed[...], basis[:, at], preferred_element_type=jnp.float32
        ).astype(quarters.dtype)
    place(quarters, points, line)
    out_ref[0] = line[:, : out_ref.shape[2]]


def synthesis(arrived, waves, points, cosine_sq, count):
    cycles, slots, columns = arrived.shape
    rows = 6 * columns // 8
    width = -(-NLON // 4 // LANES) * LANES
    return pl.pallas_call(
        functools.partial(synthesis_kernel, count),
        grid=(cycles,),
        in_specs=[
            pl.BlockSpec(memory_space=pltpu.SMEM),
            pl.BlockSpec(memory_space=pltpu.SMEM),
            pl.BlockSpec((1, slots), lambda i: (0, 0)),
            pl.BlockSpec((1, slots, columns), lambda i: (i, 0, 0)),
        ],
        out_specs=pl.BlockSpec((1, rows, NLON), lambda i: (i, 0, 0)),
        out_shape=jax.ShapeDtypeStruct((cycles, rows, NLON), jnp.bfloat16),
        scratch_shapes=[
            pltpu.VMEM((2 * slots, width), jnp.bfloat16),
            pltpu.VMEM((4 * rows, 2 * slots), jnp.bfloat16),
            pltpu.VMEM((4 * rows, width), jnp.bfloat16),
            pltpu.VMEM((rows, 4 * width + 2 * LANES), jnp.bfloat16),
        ],
    )(points, cosine_sq, waves.reshape(1, slots), arrived)


def body(vorticity, divergence, legendre, wave_of_slot, cycle_points, cos_squared):
    slots, _, count = vorticity.shape
    offset = lax.axis_index("wave") * slots
    own = lax.dynamic_slice_in_dim(wave_of_slot, offset, slots, 0)
    fourier = legendre_sums(own, vorticity, divergence, legendre)
    fourier = jnp.swapaxes(fourier, 0, 1)
    arrived = lax.all_to_all(fourier, "wave", split_axis=0, concat_axis=1, tiled=True)
    return synthesis(arrived, wave_of_slot, cycle_points, cos_squared, count)


def solution(mesh):
    return jax.shard_map(
        body,
        mesh=mesh,
        in_specs=(
            P(("member", "wave"), None, None),
            P(("member", "wave"), None, None),
            P("wave", None, None),
            P(),
            P("wave"),
            P("wave"),
        ),
        out_specs=P(("member", "wave"), None, None),
        check_vma=False,
    )
```

```python
import functools

import jax
import jax.numpy as jnp
from jax import lax
from jax.experimental import pallas as pl
from jax.experimental.pallas import tpu as pltpu
from jax.sharding import PartitionSpec as P

NLON = 5136
LANES = 128
COS = (1.0, -1 / 2, 1 / 24, -1 / 720, 1 / 40320, -1 / 3628800, 1 / 479001600,
       -1 / 87178291200, 1 / 20922789888000, -1 / 6402373705728000)
SIN = (1.0, -1 / 6, 1 / 120, -1 / 5040, 1 / 362880, -1 / 39916800, 1 / 6227020800,
       -1 / 1307674368000, 1 / 355687428096000, -1 / 121645100408832000)


def slot_block(slots):
    return max(b for b in range(1, 17) if slots % b == 0)


def degree_coefs(wave, count):
    degree = wave + lax.broadcasted_iota(jnp.int32, (wave.shape[0], count), 1)
    living = degree < count
    positive = living & (degree > 0)
    m = wave.astype(jnp.float32)
    n = degree.astype(jnp.float32)
    inverse = jnp.where(positive, -(count / 4.0) / jnp.maximum(n * (n + 1.0), 1.0), 0.0)

    def eps(x):
        return jnp.sqrt(jnp.maximum(x * x - m * m, 0.0) / jnp.maximum(4.0 * x * x - 1.0, 1.0))

    lower = jnp.where(positive, eps(n), 0.0)
    upper = jnp.where(degree + 1 < count, eps(n + 1.0), 0.0)
    live = living.astype(jnp.float32)
    return live, inverse * m, inverse * (n + 1.0) * lower, -inverse * n * upper


def slot_fourier(values, live, along, before, after, zd):
    count = values.shape[-1]
    p = values.astype(jnp.float32)
    lon = p * along
    lat = pltpu.roll(p, 1, 1) * before + pltpu.roll(p, count - 1, 1) * after
    left = jnp.concatenate([p * live, lon, lat], axis=0).astype(jnp.bfloat16)
    sums = lax.dot_general(left, zd, (((1,), (1,)), ((), ())), preferred_element_type=jnp.float32)
    rows = p.shape[0]
    lev = zd.shape[0] // 4
    plain, a, b = sums[:rows], sums[rows : 2 * rows], sums[2 * rows :]
    zr, zi, dr, di = (slice(g * lev, (g + 1) * lev) for g in range(4))
    turned = jnp.concatenate([-a[:, di], a[:, dr], -a[:, zi], a[:, zr]], axis=1)
    lane = lax.broadcasted_iota(jnp.int32, b.shape, 1)
    winds = turned + jnp.where(lane < 2 * lev, -b, b)
    return jnp.concatenate([winds, plain], axis=1)


def horner(coefs, x):
    total = jnp.full_like(x, coefs[-1])
    for c in coefs[-2::-1]:
        total = total * x + c
    return total


def turn(steps, points, per_point):
    turns = jnp.round(steps * per_point)
    theta = (steps - turns * points) * (per_point * (2.0 * jnp.pi))
    square = theta * theta
    return horner(COS, square), theta * horner(SIN, square)


def basis_columns(row, points):
    slots = row.shape[1]
    column = lambda x: jnp.broadcast_to(x, (LANES, slots)).T
    step = turn(row * float(LANES), points, 1.0 / points)
    return column(row), column(step[0]), column(step[1])


def fill_basis(columns, points, basis, first, last):
    wave, step_c, step_s = columns
    slots = wave.shape[0]
    lane = lax.broadcasted_iota(jnp.int32, (16, LANES), 1).astype(jnp.float32)
    for start in range(first, last, 16):
        rows = slice(start, start + 16)
        c, s = turn(wave[rows] * lane, points, 1.0 / points)
        cs, ss = step_c[rows], step_s[rows]
        for t in range(basis.shape[1] // LANES):
            at = slice(t * LANES, (t + 1) * LANES)
            basis[rows, at] = c.astype(basis.dtype)
            basis[slots + start : slots + start + 16, at] = s.astype(basis.dtype)
            c, s = c * cs - s * ss, s * cs + c * ss


def fill_fields(arrived, wave, points, cosine_sq, count, packed):
    x = arrived.astype(jnp.float32).T
    lev = x.shape[0] // 8
    ur, ui, vr, vi, zr, zi, dr, di = (x[g * lev : (g + 1) * lev] for g in range(8))
    slots = wave.shape[1]
    m = wave.astype(jnp.float32)
    q = m * (4.0 / count)
    over = 1.0 / jnp.full_like(m, cosine_sq)
    ulr, uli, vlr, vli = -q * ui, q * ur, -q * vi, q * vr
    fields = (
        (ur, ui), (vr, vi), (ulr, uli), (vlr, vli),
        (vlr * over - zr, vli * over - zi), (dr - ulr * over, di - uli * over),
    )
    weight = jnp.where(2 * wave < points, jnp.where(wave == 0, 1.0, 2.0), 0.0)
    for f, (re, im) in enumerate(fields):
        a, b = re * weight, -im * weight
        for j in range(4):
            phase = (wave * j) & 3
            c = jnp.where(phase == 0, 1.0, jnp.where(phase == 2, -1.0, 0.0))
            s = jnp.where(phase == 1, 1.0, jnp.where(phase == 3, -1.0, 0.0))
            start = (j * len(fields) + f) * lev
            rows = slice(start, start + lev)
            packed[rows, :slots] = (a * c + b * s).astype(packed.dtype)
            packed[rows, slots:] = (b * c - a * s).astype(packed.dtype)


def place(quarters, points, line):
    rows = quarters.shape[0] // 4
    tiles = quarters.shape[1] // LANES
    quarter = points // 4
    lane = lax.broadcasted_iota(jnp.int32, (rows, LANES), 1)
    line[...] = jnp.zeros_like(line)
    for j in range(4):
        offset = quarter * j
        base = pl.multiple_of(offset // LANES * LANES, LANES)
        shift = offset - base
        previous = jnp.zeros((rows, LANES), jnp.float32)
        for t in range(tiles + 1):
            rolled = jnp.zeros((rows, LANES), jnp.float32)
            if t < tiles:
                tile = quarters[j * rows : (j + 1) * rows, t * LANES : (t + 1) * LANES]
                tile = jnp.where(lane + t * LANES < quarter, tile.astype(jnp.float32), 0.0)
                rolled = pltpu.roll(tile, shift, 1)
            moved = jnp.where(lane < shift, previous, rolled).astype(line.dtype)
            at = pl.ds(pl.multiple_of(base + t * LANES, LANES), LANES)
            line[:, at] = line[:, at] + moved
            previous = rolled


def exchange_kernel(
    points_ref, cosine_ref, slots_ref, wave_ref, zeta_ref, delta_ref, values_ref, quarters_ref,
    sums, sent, held, basis, packed, send_sem, recv_sem,
):
    step = pl.program_id(0)
    cycles, devices, blocks, sb, columns = held.shape
    count = zeta_ref.shape[-1]
    me = lax.axis_index("wave")
    barrier = pltpu.get_barrier_semaphore()

    def copy(block, off, cycle):
        to = lax.rem(me + off, devices)
        return pltpu.make_async_remote_copy(
            src_ref=sent.at[block, to * cycles + cycle],
            dst_ref=held.at[cycle, me, block],
            send_sem=send_sem.at[block, cycle, off - 1],
            recv_sem=recv_sem.at[block, cycle, off - 1],
            device_id={"wave": to},
            device_id_type=pl.DeviceIdType.MESH,
        )

    def send(block):
        for cycle in range(cycles):
            pl.loop(1, devices)(lambda off: copy(block, off, cycle).start())

    @pl.when(step == 0)
    def _():
        @pl.loop(1, devices)
        def _(off):
            pl.semaphore_signal(
                barrier, inc=1, device_id={"wave": lax.rem(me + off, devices)},
                device_id_type=pl.DeviceIdType.MESH,
            )

    @pl.when(step == 1)
    def _():
        pl.semaphore_wait(barrier, devices - 1)

    @pl.when(step > 0)
    def _():
        send(step - 1)

    first = me * (blocks * sb) + step * sb
    row = lax.broadcasted_iota(jnp.int32, (sb, 1), 0)
    waves = jnp.zeros((sb, 1), jnp.int32)
    for s in range(sb):
        waves = jnp.where(row == s, slots_ref[first + s], waves)
    coefs = degree_coefs(waves, count)
    rows = values_ref.shape[1]
    for s in range(sb):
        zd = jnp.concatenate([zeta_ref[s], delta_ref[s]], axis=0)
        out = slot_fourier(values_ref[s], *(c[s : s + 1] for c in coefs), zd)
        sums[pl.ds(s, rows, sb), :] = out
    sent[step] = sums[...].astype(sent.dtype).reshape(rows, sb, columns)

    @pl.when(step == blocks - 1)
    def _():
        wave = wave_ref[...].reshape(1, -1)
        slots = wave.shape[1]
        for cycle in range(cycles):
            points = points_ref[cycle]
            points_f = jnp.full((1, 1), points, jnp.int32).astype(jnp.float32)
            cols = basis_columns(wave.astype(jnp.float32), points_f)
            early = slots // 4 // 16 * 16
            fill_basis(cols, points_f, basis, 0, early)
            if cycle == 0:
                send(blocks - 1)
            fill_basis(cols, points_f, basis, early, slots)
            if cycle == 0:
                for c in range(cycles):
                    for block in range(blocks):
                        held[c, me, block] = sent[block, me * cycles + c]

                        @pl.loop(1, devices)
                        def _(off):
                            copy(block, off, c).wait_recv()
            arrived = held[cycle].reshape(slots, columns)
            fill_fields(arrived, wave, points, cosine_ref[cycle], count, packed)
            width = basis.shape[1]
            for start in range(0, width, 256):
                at = slice(start, min(start + 256, width))
                quarters_ref[cycle, :, at] = jnp.dot(
                    packed[...], basis[:, at], preferred_element_type=jnp.float32
                ).astype(quarters_ref.dtype)
        for c in range(cycles):
            for block in range(blocks):

                @pl.loop(1, devices)
                def _(off):
                    copy(block, off, c).wait_send()


def cycle_quarters(points, cosine_sq, wave_of_slot, vorticity, divergence, legendre):
    slots, half, count = vorticity.shape
    lines = legendre.shape[1]
    cycles = points.shape[0]
    devices = lines // cycles
    columns = 4 * half
    rows = 6 * half
    width = -(-NLON // 4 // LANES) * LANES
    sb = slot_block(slots)
    blocks = slots // sb
    block = lambda n: pl.BlockSpec((sb, n, count), lambda i: (i, 0, 0))
    smem = pl.BlockSpec(memory_space=pltpu.SMEM)
    sem = pltpu.SemaphoreType.DMA((blocks, cycles, devices - 1))
    return pl.pallas_call(
        exchange_kernel,
        grid=(blocks,),
        in_specs=[
            smem, smem, smem, pl.BlockSpec(memory_space=pltpu.VMEM),
            block(half), block(half), block(lines),
        ],
        out_specs=pl.BlockSpec((cycles, 2 * rows, width), lambda i: (0, 0, 0)),
        out_shape=jax.ShapeDtypeStruct((cycles, 2 * rows, width), jnp.bfloat16),
        scratch_shapes=[
            pltpu.VMEM((lines * sb, columns), jnp.float32),
            pltpu.VMEM((blocks, lines, sb, columns), jnp.bfloat16),
            pltpu.VMEM((cycles, devices, blocks, sb, columns), jnp.bfloat16),
            pltpu.VMEM((2 * devices * slots, width), jnp.bfloat16),
            pltpu.VMEM((2 * rows, 2 * devices * slots), jnp.bfloat16),
            sem,
            sem,
        ],
        compiler_params=pltpu.CompilerParams(collective_id=0, has_side_effects=True),
    )(points, cosine_sq, wave_of_slot, wave_of_slot, vorticity, divergence, legendre)


def place_kernel(points_ref, quarters_ref, out_ref, line):
    place(quarters_ref.at[0], points_ref[pl.program_id(0)], line)
    out_ref[0] = line[:, : out_ref.shape[2]]


def placed(quarters, points):
    cycles, rows, width = quarters.shape
    rows = rows // 4
    return pl.pallas_call(
        place_kernel,
        grid=(cycles,),
        in_specs=[
            pl.BlockSpec(memory_space=pltpu.SMEM),
            pl.BlockSpec((1, 4 * rows, width), lambda i: (i, 0, 0)),
        ],
        out_specs=pl.BlockSpec((1, rows, NLON), lambda i: (i, 0, 0)),
        out_shape=jax.ShapeDtypeStruct((cycles, rows, NLON), jnp.bfloat16),
        scratch_shapes=[pltpu.VMEM((rows, 4 * width + 2 * LANES), jnp.bfloat16)],
    )(points, quarters)


def body(vorticity, divergence, legendre, wave_of_slot, cycle_points, cos_squared):
    quarters = cycle_quarters(
        cycle_points, cos_squared, wave_of_slot, vorticity, divergence, legendre
    )
    return placed(quarters, cycle_points)


def solution(mesh):
    return jax.shard_map(
        body,
        mesh=mesh,
        in_specs=(
            P(("member", "wave"), None, None),
            P(("member", "wave"), None, None),
            P("wave", None, None),
            P(),
            P("wave"),
            P("wave"),
        ),
        out_specs=P(("member", "wave"), None, None),
        check_vma=False,
    )
```

```python
import functools

import jax
import jax.numpy as jnp
from jax import lax
from jax.experimental import pallas as pl
from jax.experimental.pallas import tpu as pltpu
from jax.sharding import PartitionSpec as P

NLON = 5136
LANES = 128
COS = (1.0, -1 / 2, 1 / 24, -1 / 720, 1 / 40320, -1 / 3628800, 1 / 479001600,
       -1 / 87178291200, 1 / 20922789888000, -1 / 6402373705728000)
SIN = (1.0, -1 / 6, 1 / 120, -1 / 5040, 1 / 362880, -1 / 39916800, 1 / 6227020800,
       -1 / 1307674368000, 1 / 355687428096000, -1 / 121645100408832000)


def slot_block(slots):
    return max(b for b in range(1, 17) if slots % b == 0)


def degree_coefs(wave, count):
    degree = wave + lax.broadcasted_iota(jnp.int32, (wave.shape[0], count), 1)
    living = degree < count
    positive = living & (degree > 0)
    m = wave.astype(jnp.float32)
    n = degree.astype(jnp.float32)
    inverse = jnp.where(positive, -(count / 4.0) / jnp.maximum(n * (n + 1.0), 1.0), 0.0)

    def eps(x):
        return jnp.sqrt(jnp.maximum(x * x - m * m, 0.0) / jnp.maximum(4.0 * x * x - 1.0, 1.0))

    lower = jnp.where(positive, eps(n), 0.0)
    upper = jnp.where(degree + 1 < count, eps(n + 1.0), 0.0)
    live = living.astype(jnp.float32)
    return live, inverse * m, inverse * (n + 1.0) * lower, -inverse * n * upper


def slot_fourier(values, live, along, before, after, zd):
    count = values.shape[-1]
    p = values.astype(jnp.float32)
    lon = p * along
    lat = pltpu.roll(p, 1, 1) * before + pltpu.roll(p, count - 1, 1) * after
    left = jnp.concatenate([p * live, lon, lat], axis=0).astype(jnp.bfloat16)
    sums = lax.dot_general(left, zd, (((1,), (1,)), ((), ())), preferred_element_type=jnp.float32)
    rows = p.shape[0]
    lev = zd.shape[0] // 4
    plain, a, b = sums[:rows], sums[rows : 2 * rows], sums[2 * rows :]
    zr, zi, dr, di = (slice(g * lev, (g + 1) * lev) for g in range(4))
    turned = jnp.concatenate([-a[:, di], a[:, dr], -a[:, zi], a[:, zr]], axis=1)
    lane = lax.broadcasted_iota(jnp.int32, b.shape, 1)
    winds = turned + jnp.where(lane < 2 * lev, -b, b)
    return jnp.concatenate([winds, plain], axis=1)


def horner(coefs, x):
    total = jnp.full_like(x, coefs[-1])
    for c in coefs[-2::-1]:
        total = total * x + c
    return total


def turn(steps, points, per_point):
    turns = jnp.round(steps * per_point)
    theta = (steps - turns * points) * (per_point * (2.0 * jnp.pi))
    square = theta * theta
    return horner(COS, square), theta * horner(SIN, square)


def basis_columns(row, points):
    slots = row.shape[1]
    column = lambda x: jnp.broadcast_to(x, (LANES, slots)).T
    step = turn(row * float(LANES), points, 1.0 / points)
    return column(row), column(step[0]), column(step[1])


def fill_basis(columns, points, basis, first, last):
    wave, step_c, step_s = columns
    slots = wave.shape[0]
    lane = lax.broadcasted_iota(jnp.int32, (16, LANES), 1).astype(jnp.float32)
    for start in range(first, last, 16):
        rows = slice(start, start + 16)
        c, s = turn(wave[rows] * lane, points, 1.0 / points)
        cs, ss = step_c[rows], step_s[rows]
        for t in range(basis.shape[1] // LANES):
            at = slice(t * LANES, (t + 1) * LANES)
            basis[rows, at] = c.astype(basis.dtype)
            basis[slots + start : slots + start + 16, at] = s.astype(basis.dtype)
            c, s = c * cs - s * ss, s * cs + c * ss


def fill_fields(arrived, wave, points, cosine_sq, count, packed):
    x = arrived.astype(jnp.float32).T
    lev = x.shape[0] // 8
    ur, ui, vr, vi, zr, zi, dr, di = (x[g * lev : (g + 1) * lev] for g in range(8))
    slots = wave.shape[1]
    m = wave.astype(jnp.float32)
    q = m * (4.0 / count)
    over = 1.0 / jnp.full_like(m, cosine_sq)
    ulr, uli, vlr, vli = -q * ui, q * ur, -q * vi, q * vr
    fields = (
        (ur, ui), (vr, vi), (ulr, uli), (vlr, vli),
        (vlr * over - zr, vli * over - zi), (dr - ulr * over, di - uli * over),
    )
    weight = jnp.where(2 * wave < points, jnp.where(wave == 0, 1.0, 2.0), 0.0)
    for f, (re, im) in enumerate(fields):
        a, b = re * weight, -im * weight
        for j in range(4):
            phase = (wave * j) & 3
            c = jnp.where(phase == 0, 1.0, jnp.where(phase == 2, -1.0, 0.0))
            s = jnp.where(phase == 1, 1.0, jnp.where(phase == 3, -1.0, 0.0))
            start = (j * len(fields) + f) * lev
            rows = slice(start, start + lev)
            packed[rows, :slots] = (a * c + b * s).astype(packed.dtype)
            packed[rows, slots:] = (b * c - a * s).astype(packed.dtype)


def place(quarters, points, line):
    rows = quarters.shape[0] // 4
    tiles = quarters.shape[1] // LANES
    quarter = points // 4
    lane = lax.broadcasted_iota(jnp.int32, (rows, LANES), 1)
    line[...] = jnp.zeros_like(line)
    for j in range(4):
        offset = quarter * j
        base = pl.multiple_of(offset // LANES * LANES, LANES)
        shift = offset - base
        previous = jnp.zeros((rows, LANES), jnp.float32)
        for t in range(tiles + 1):
            rolled = jnp.zeros((rows, LANES), jnp.float32)
            if t < tiles:
                tile = quarters[j * rows : (j + 1) * rows, t * LANES : (t + 1) * LANES]
                tile = jnp.where(lane + t * LANES < quarter, tile.astype(jnp.float32), 0.0)
                rolled = pltpu.roll(tile, shift, 1)
            moved = jnp.where(lane < shift, previous, rolled).astype(line.dtype)
            at = pl.ds(pl.multiple_of(base + t * LANES, LANES), LANES)
            line[:, at] = line[:, at] + moved
            previous = rolled


def send_groups(blocks):
    return [(0, (blocks + 1) // 2), ((blocks + 1) // 2, blocks)]


def exchange_kernel(
    groups,     points_ref, cosine_ref, slots_ref, wave_ref, zeta_ref, delta_ref, values_ref, quarters_ref,
    sums, sent, held, basis, packed, send_sem, recv_sem,
):
    step = pl.program_id(0)
    cycles, devices, blocks, sb, columns = held.shape
    count = zeta_ref.shape[-1]
    me = lax.axis_index("wave")
    barrier = pltpu.get_barrier_semaphore()

    def copy(group, off, cycle):
        start, stop = groups[group]
        to = lax.rem(me + off, devices)
        return pltpu.make_async_remote_copy(
            src_ref=sent.at[to * cycles + cycle, start:stop],
            dst_ref=held.at[cycle, me, start:stop],
            send_sem=send_sem.at[group, cycle, off - 1],
            recv_sem=recv_sem.at[group, cycle, off - 1],
            device_id={"wave": to},
            device_id_type=pl.DeviceIdType.MESH,
        )

    def each(group, act):
        for cycle in range(cycles):
            pl.loop(1, devices)(lambda off: act(copy(group, off, cycle)))

    def send(group):
        if group == 0:
            pl.semaphore_wait(barrier, devices - 1)
        each(group, lambda c: c.start())

    @pl.when(step == 0)
    def _():
        @pl.loop(1, devices)
        def _(off):
            pl.semaphore_signal(
                barrier, inc=1, device_id={"wave": lax.rem(me + off, devices)},
                device_id_type=pl.DeviceIdType.MESH,
            )

    for group, (_, stop) in enumerate(groups[:-1]):
        pl.when(step == stop)(functools.partial(send, group))

    first = me * (blocks * sb) + step * sb
    row = lax.broadcasted_iota(jnp.int32, (sb, 1), 0)
    waves = jnp.zeros((sb, 1), jnp.int32)
    for s in range(sb):
        waves = jnp.where(row == s, slots_ref[first + s], waves)
    coefs = degree_coefs(waves, count)
    rows = values_ref.shape[1]
    for s in range(sb):
        zd = jnp.concatenate([zeta_ref[s], delta_ref[s]], axis=0)
        out = slot_fourier(values_ref[s], *(c[s : s + 1] for c in coefs), zd)
        sums[pl.ds(s, rows, sb), :] = out
    sent[:, step] = sums[...].astype(sent.dtype).reshape(rows, sb, columns)

    @pl.when(step == blocks - 1)
    def _():
        wave = wave_ref[...].reshape(1, -1)
        slots = wave.shape[1]
        for cycle in range(cycles):
            points = points_ref[cycle]
            points_f = jnp.full((1, 1), points, jnp.int32).astype(jnp.float32)
            cols = basis_columns(wave.astype(jnp.float32), points_f)
            early = slots // 4 // 16 * 16
            fill_basis(cols, points_f, basis, 0, early)
            if cycle == 0:
                send(len(groups) - 1)
            fill_basis(cols, points_f, basis, early, slots)
            if cycle == 0:
                for c in range(cycles):
                    held[c, me] = sent[me * cycles + c]
                for group in range(len(groups)):
                    each(group, lambda c: c.wait_recv())
            arrived = held[cycle].reshape(slots, columns)
            fill_fields(arrived, wave, points, cosine_ref[cycle], count, packed)
            width = basis.shape[1]
            for start in range(0, width, 256):
                at = slice(start, min(start + 256, width))
                quarters_ref[cycle, :, at] = jnp.dot(
                    packed[...], basis[:, at], preferred_element_type=jnp.float32
                ).astype(quarters_ref.dtype)
        for group in range(len(groups)):
            each(group, lambda c: c.wait_send())


def cycle_quarters(points, cosine_sq, wave_of_slot, vorticity, divergence, legendre):
    slots, half, count = vorticity.shape
    lines = legendre.shape[1]
    cycles = points.shape[0]
    devices = lines // cycles
    columns = 4 * half
    rows = 6 * half
    width = -(-NLON // 4 // LANES) * LANES
    sb = slot_block(slots)
    blocks = slots // sb
    block = lambda n: pl.BlockSpec((sb, n, count), lambda i: (i, 0, 0))
    smem = pl.BlockSpec(memory_space=pltpu.SMEM)
    groups = send_groups(blocks)
    sem = pltpu.SemaphoreType.DMA((len(groups), cycles, devices - 1))
    return pl.pallas_call(
        functools.partial(exchange_kernel, groups),
        grid=(blocks,),
        in_specs=[
            smem, smem, smem, pl.BlockSpec(memory_space=pltpu.VMEM),
            block(half), block(half), block(lines),
        ],
        out_specs=pl.BlockSpec((cycles, 2 * rows, width), lambda i: (0, 0, 0)),
        out_shape=jax.ShapeDtypeStruct((cycles, 2 * rows, width), jnp.bfloat16),
        scratch_shapes=[
            pltpu.VMEM((lines * sb, columns), jnp.float32),
            pltpu.VMEM((lines, blocks, sb, columns), jnp.bfloat16),
            pltpu.VMEM((cycles, devices, blocks, sb, columns), jnp.bfloat16),
            pltpu.VMEM((2 * devices * slots, width), jnp.bfloat16),
            pltpu.VMEM((2 * rows, 2 * devices * slots), jnp.bfloat16),
            sem,
            sem,
        ],
        compiler_params=pltpu.CompilerParams(collective_id=0, has_side_effects=True),
    )(points, cosine_sq, wave_of_slot, wave_of_slot, vorticity, divergence, legendre)


def place_kernel(points_ref, quarters_ref, out_ref, line):
    place(quarters_ref.at[0], points_ref[pl.program_id(0)], line)
    out_ref[0] = line[:, : out_ref.shape[2]]


def placed(quarters, points):
    cycles, rows, width = quarters.shape
    rows = rows // 4
    return pl.pallas_call(
        place_kernel,
        grid=(cycles,),
        in_specs=[
            pl.BlockSpec(memory_space=pltpu.SMEM),
            pl.BlockSpec((1, 4 * rows, width), lambda i: (i, 0, 0)),
        ],
        out_specs=pl.BlockSpec((1, rows, NLON), lambda i: (i, 0, 0)),
        out_shape=jax.ShapeDtypeStruct((cycles, rows, NLON), jnp.bfloat16),
        scratch_shapes=[pltpu.VMEM((rows, 4 * width + 2 * LANES), jnp.bfloat16)],
    )(points, quarters)


def body(vorticity, divergence, legendre, wave_of_slot, cycle_points, cos_squared):
    quarters = cycle_quarters(
        cycle_points, cos_squared, wave_of_slot, vorticity, divergence, legendre
    )
    return placed(quarters, cycle_points)


def solution(mesh):
    return jax.shard_map(
        body,
        mesh=mesh,
        in_specs=(
            P(("member", "wave"), None, None),
            P(("member", "wave"), None, None),
            P("wave", None, None),
            P(),
            P("wave"),
            P("wave"),
        ),
        out_specs=P(("member", "wave"), None, None),
        check_vma=False,
    )
```
